256 devices in a mesh: tm: 128 (over x_hi, y, z, core), pb: 2 (over x_lo).
Axes of the slice: x: 4 (x_hi: 2, x_lo: 2; x = x_hi * 2 + x_lo), y: 4, z: 8, core: 2. Of those that a mesh axis runs over, the one named last changes fastest.
Arguments:
- queries: bfloat16 [32768, 768], P(('tm', 'pb')), may hold values from -64 to 64
- corpus: bfloat16 [2097152, 768], P(('tm', 'pb')), may hold values from -40 to 40
- window_start: int32 [32768, 2], P(('tm', 'pb')), may hold values from 0 to 2097150, as said below
- window_end: int32 [32768, 2], P(('tm', 'pb')), may hold values from 2 to 2097152, as said below
Outputs:
- pooled: bfloat16 [32768, 2, 768], P(('tm', 'pb'))
- log_mass: float32 [32768, 2], P(('tm', 'pb'))
- mean_score: float32 [32768, 2], P(('tm', 'pb'))
The draws below stay inside these ranges and needn't reach their ends.
Inputs may be any that keep to these rules, and one draw needn't show every extreme that they name: `window_start`: for query q both windows are nonempty and lie within documents (q // 128 - 1) * 8192 to (q // 128 + 2) * 8192 - 1, that is the time block of q and the blocks just before and after it. window_end[q, w] > window_start[q, w], and window_end[q, w] <= (q // 128 + 2) * 8192.
All inputs are finite; a program needn't handle non-finite values.
Results may differ from the reference program's by a relative error of at most 0.0051.
Values may be sent and summed in bfloat16 or wider, within the bound.
A program may use at most 128 MiB of HBM per device.

```python
import math
from functools import reduce
import jax
import jax.numpy as jnp
from jax import lax

D = 768
Q_DEV = 128
DOC_DEV = 8192
NQ = 32768
NDOC = 2097152
N_TM = 128
N_PB = 2


def window_bounds(key):
    key_anchor, key_back, key_ahead = jax.random.split(jax.random.fold_in(key, 101), 3)
    owner_block = jnp.arange(NQ, dtype=jnp.int32) // Q_DEV
    anchor = owner_block * DOC_DEV + 2 * jax.random.randint(key_anchor, (NQ,), 0, DOC_DEV // 2) + 1
    behind = jax.random.randint(key_back, (NQ, 2), 1, DOC_DEV + 1)
    forward = jax.random.randint(key_ahead, (NQ, 2), 0, DOC_DEV + 1)
    first_doc = jnp.maximum(anchor[:, None] - behind, 0)
    stop_doc = jnp.minimum(anchor[:, None] + forward + 1, NDOC)
    return (first_doc.astype(jnp.int32), stop_doc.astype(jnp.int32))


def corpus_rows(key):
    key_base = jax.random.fold_in(jax.random.fold_in(key, 202), 0)
    values = jax.random.normal(key_base, (NDOC, D), jnp.float32)
    return jnp.clip(values, -40.0, 40.0)


def draw_corpus(key, part):
    return corpus_rows(key).astype(jnp.bfloat16)


def draw_queries(key, part):
    drawn = jax.random.normal(jax.random.fold_in(key, 303), (NQ, D), jnp.float32)
    return jnp.clip(drawn, -64.0, 64.0).astype(jnp.bfloat16)


def draw_window_start(key, part):
    first_doc, stop_doc = window_bounds(key)
    return first_doc


def draw_window_end(key, part):
    first_doc, stop_doc = window_bounds(key)
    return stop_doc


def setup_inputs(seed: int = 0) -> dict:
    keys = jax.random.split(jax.random.key(seed), 5)
    return {
        "queries": draw_queries(jax.random.fold_in(keys[4], 71), 0),
        "corpus": draw_corpus(jax.random.fold_in(keys[4], 71), 0),
        "window_start": draw_window_start(jax.random.fold_in(keys[4], 71), 0),
        "window_end": draw_window_end(jax.random.fold_in(keys[4], 71), 0),
    }


NEG_FILL = -1e+30
SCORE_SCALE = 3.0

def block_state(query_rows, first_doc, stop_doc, block, start_doc):
    scores = lax.dot_general(query_rows, block, (((1,), (1,)), ((), ())), preferred_element_type=jnp.float32)
    scores = scores * (SCORE_SCALE / math.sqrt(block.shape[1]))
    doc_index = start_doc + jnp.arange(block.shape[0], dtype=jnp.int32)
    maxima, totals, parts, score_sums, counts = ([], [], [], [], [])
    for window in range(2):
        inside = (doc_index[None, :] >= first_doc[:, window:window + 1]) & (doc_index[None, :] < stop_doc[:, window:window + 1])
        window_max = lax.optimization_barrier(jnp.max(jnp.where(inside, scores, NEG_FILL), axis=1))
        weights = jnp.where(inside, jnp.exp(scores - window_max[:, None]), 0.0)
        maxima.append(window_max)
        totals.append(lax.optimization_barrier(jnp.sum(weights, axis=1)))
        parts.append(jnp.dot(weights.astype(jnp.bfloat16), block, preferred_element_type=jnp.float32).astype(jnp.bfloat16))
        score_sums.append(lax.optimization_barrier(jnp.sum(jnp.where(inside, scores, 0.0), axis=1)))
        counts.append(lax.optimization_barrier(jnp.sum(inside.astype(jnp.float32), axis=1)))
    return (jnp.stack(maxima, 1), jnp.stack(totals, 1), jnp.stack(parts, 1), jnp.stack(score_sums, 1), jnp.stack(counts, 1))

def combine(states):
    tops = [jnp.where(member[4] > 0, member[0], NEG_FILL) for member in states]
    overall = reduce(jnp.maximum, tops)
    rescale = [jnp.exp(value - overall) for value in tops]
    denominator = reduce(jnp.add, [factor * member[1] for factor, member in zip(rescale, states)])
    weighted = reduce(jnp.add, [factor[..., None] * member[2].astype(jnp.float32) for factor, member in zip(rescale, states)])
    pooled = (weighted / denominator[..., None]).astype(jnp.bfloat16)
    log_mass = overall + jnp.log(denominator)
    mean_score = reduce(jnp.add, [member[3] for member in states]) / reduce(jnp.add, [member[4] for member in states])
    return (pooled, log_mass, mean_score)

def reference(queries, corpus, window_start, window_end):
    blocks = N_TM * N_PB
    feature_width = corpus.shape[1]
    padding = jnp.zeros((DOC_DEV, feature_width), corpus.dtype)
    padded = jnp.concatenate([padding, corpus, padding], axis=0)

    def per_owner(owner_block):
        query_rows = lax.dynamic_slice_in_dim(queries, owner_block * Q_DEV, Q_DEV, 0)
        first_doc = lax.dynamic_slice_in_dim(window_start, owner_block * Q_DEV, Q_DEV, 0)
        stop_doc = lax.dynamic_slice_in_dim(window_end, owner_block * Q_DEV, Q_DEV, 0)
        states = []
        for offset in (-1, 0, 1):
            block = lax.dynamic_slice_in_dim(padded, (owner_block + offset + 1) * DOC_DEV, DOC_DEV, 0)
            start_doc = ((owner_block + offset) * DOC_DEV).astype(jnp.int32)
            states.append(block_state(query_rows, first_doc, stop_doc, block, start_doc))
        return combine(states)
    pooled, log_mass, mean_score = lax.map(per_owner, jnp.arange(blocks, dtype=jnp.int32))
    return (pooled.reshape(blocks * Q_DEV, 2, feature_width), log_mass.reshape(blocks * Q_DEV, 2), mean_score.reshape(blocks * Q_DEV, 2))
```

```python
import functools
import math

import jax
import jax.numpy as jnp
from jax import lax
from jax.experimental import pallas as pl
from jax.experimental.pallas import tpu as pltpu
from jax.sharding import PartitionSpec as P

NEG_FILL = -1e30
SCORE_SCALE = 3.0
LOG2E = math.log2(math.e)
LN2 = math.log(2.0)
MESH = pl.DeviceIdType.MESH

CHUNK = 1024


def fold_rows(op, x):
    rows, cols = x.shape
    return op(x.reshape(rows // 8, 8, cols), axis=0)


def kernel(
    n_dev,
    n_pb,
    scale,
    q_hbm,
    c_hbm,
    start_hbm,
    stop_hbm,
    pooled_ref,
    log_mass_ref,
    mean_ref,
    c_v,
    c_t,
    xm,
    q_v,
    q_in,
    q_t,
    w_v,
    w_in,
    maxs,
    sums,
    tots,
    acc,
    acc_own,
    parts_out,
    parts_in,
    stats_out,
    stats_in,
    c_sem,
    local_sem,
    q_send,
    q_recv,
    w_send,
    w_recv,
    p_send,
    p_recv,
    s_send,
    s_recv,
):
    n_q, dim = q_hbm.shape
    n_doc = c_hbm.shape[0]
    chunks = n_doc // CHUNK
    me = lax.axis_index("tm") * n_pb + lax.axis_index("pb")

    def coords(pos):
        return (pos // n_pb, pos % n_pb)

    prior = coords((me + n_dev - 1) % n_dev)
    following = coords((me + 1) % n_dev)

    def c_copy(i):
        rows = pl.ds(pl.multiple_of(i * CHUNK, CHUNK), CHUNK)
        return pltpu.make_async_copy(c_hbm.at[rows, :], c_v.at[rows, :], c_sem.at[i])

    q_copy = pltpu.make_async_copy(q_hbm, q_v, local_sem.at[0])
    start_copy = pltpu.make_async_copy(start_hbm, w_v.at[0], local_sem.at[1])
    stop_copy = pltpu.make_async_copy(stop_hbm, w_v.at[1], local_sem.at[2])
    q_copy.start()
    start_copy.start()
    stop_copy.start()
    lax.fori_loop(0, chunks, lambda i, _: (c_copy(i).start(), 0)[1], 0)

    barrier = pltpu.get_barrier_semaphore()
    for neighbour in (prior, following):
        pl.semaphore_signal(barrier, inc=1, device_id=neighbour, device_id_type=MESH)
    pl.semaphore_wait(barrier, 2)
    q_copy.wait()
    start_copy.wait()
    stop_copy.wait()

    out_copies, q_copies, p_copies, s_copies = [], {}, {}, {}
    for slot, neighbour in ((1, prior), (0, following)):
        for src, dst, send, recv in (
            (w_v, w_in, w_send, w_recv),
            (q_v, q_in, q_send, q_recv),
        ):
            copy = pltpu.make_async_remote_copy(
                src_ref=src,
                dst_ref=dst.at[slot],
                send_sem=send.at[slot],
                recv_sem=recv.at[slot],
                device_id=neighbour,
                device_id_type=MESH,
            )
            copy.start()
            out_copies.append(copy)
            q_copies.setdefault(slot, []).append(copy)

    start_doc = me * n_doc

    def scores_pass(rhs, bounds, targets, base, cols, transpose):
        width = rhs.shape[1]
        for w in range(2):
            maxs[base + w, :, :width] = jnp.full((8, width), NEG_FILL, jnp.float32)
            sums[base + w, :, :width] = jnp.zeros((8, width), jnp.float32)

        def body(i, carry):
            rows = pl.ds(pl.multiple_of(i * CHUNK, CHUNK), CHUNK)
            if transpose:
                c_copy(i).wait()
            block = c_v[rows, :]
            x = jnp.dot(block, rhs[...], preferred_element_type=jnp.float32) * (scale * LOG2E)
            if transpose:
                c_t[:, rows] = block.T
            doc = lax.broadcasted_iota(jnp.int32, (CHUNK, width), 0)
            for w in range(2):
                low, size = bounds[w]
                offset = (i * CHUNK - low).astype(jnp.int32)
                inside = (doc + offset).astype(jnp.uint32) < size.astype(jnp.uint32)
                kept = jnp.where(inside, x, NEG_FILL)
                xm[targets[w], rows, cols[w]] = kept
                maxs[base + w, :, :width] = jnp.maximum(
                    maxs[base + w, :, :width], fold_rows(jnp.max, kept)
                )
                sums[base + w, :, :width] += fold_rows(jnp.sum, jnp.where(inside, x, 0.0))
            return carry

        lax.fori_loop(0, chunks, body, 0)

    def parts_pass(source, top, out):
        out[...] = jnp.zeros_like(out)
        tots[...] = jnp.zeros_like(tots)

        def body(i, carry):
            rows = pl.ds(pl.multiple_of(i * CHUNK, CHUNK), CHUNK)
            weights = jnp.exp2(xm[source, rows, :] - top)
            tots[...] += fold_rows(jnp.sum, weights)
            out[...] += jnp.dot(
                c_t[:, rows], weights.astype(jnp.bfloat16), preferred_element_type=jnp.float32
            )
            return carry

        lax.fori_loop(0, chunks, body, 0)
        return jnp.sum(tots[...], axis=0, keepdims=True)

    q_t[:, pl.ds(0, n_q)] = q_v[...].T
    own_bounds = []
    for w in range(2):
        low = w_v[0, w : w + 1, :]
        own_bounds.append((low - start_doc, w_v[1, w : w + 1, :] - low))
    scores_pass(
        q_t.at[:, pl.ds(0, n_q)],
        own_bounds,
        (0, 0),
        0,
        (pl.ds(0, n_q), pl.ds(n_q, n_q)),
        True,
    )
    own_top = [jnp.max(maxs[w, :, :n_q], axis=0, keepdims=True) for w in range(2)]
    own_sum = [jnp.sum(sums[w, :, :n_q], axis=0, keepdims=True) for w in range(2)]
    own_tot = parts_pass(0, jnp.concatenate(own_top, axis=1), acc_own)

    for slot in range(2):
        for copy in q_copies[slot]:
            copy.wait_recv()
    for slot in range(2):
        q_t[:, pl.ds(slot * n_q, n_q)] = q_in[slot].T
    bounds = []
    for w in range(2):
        low = jnp.concatenate([w_in[slot, 0, w : w + 1, :] for slot in range(2)], axis=1)
        stop = jnp.concatenate([w_in[slot, 1, w : w + 1, :] for slot in range(2)], axis=1)
        bounds.append((low - start_doc, stop - low))
    scores_pass(q_t, bounds, (0, 1), 0, (pl.ds(0, 2 * n_q),) * 2, False)
    back = (prior, following)
    for w in range(2):
        top = jnp.max(maxs[w], axis=0, keepdims=True)
        total = jnp.sum(sums[w], axis=0, keepdims=True)
        mass = parts_pass(w, top, acc)
        for slot in range(2):
            half = slice(slot * n_q, (slot + 1) * n_q)
            stats_out[slot, 3 * w : 3 * w + 1, :] = top[:, half]
            stats_out[slot, 3 * w + 1 : 3 * w + 2, :] = mass[:, half]
            stats_out[slot, 3 * w + 2 : 3 * w + 3, :] = total[:, half]
            parts_out[slot, w] = acc[:, half].astype(jnp.bfloat16)
        for slot in range(2):
            copy = pltpu.make_async_remote_copy(
                src_ref=parts_out.at[slot, w],
                dst_ref=parts_in.at[1 - slot, w],
                send_sem=p_send.at[slot, w],
                recv_sem=p_recv.at[1 - slot, w],
                device_id=back[slot],
                device_id_type=MESH,
            )
            copy.start()
            out_copies.append(copy)
            p_copies[1 - slot, w] = copy
    for slot in range(2):
        copy = pltpu.make_async_remote_copy(
            src_ref=stats_out.at[slot],
            dst_ref=stats_in.at[1 - slot],
            send_sem=s_send.at[slot],
            recv_sem=s_recv.at[1 - slot],
            device_id=back[slot],
            device_id_type=MESH,
        )
        copy.start()
        out_copies.append(copy)
        s_copies[1 - slot] = copy

    for slot in range(2):
        s_copies[slot].wait_recv()
    for w in range(2):
        half = slice(w * n_q, (w + 1) * n_q)
        tops = [own_top[w]] + [stats_in[slot, 3 * w : 3 * w + 1, :] for slot in range(2)]
        masses = [own_tot[:, half]] + [
            stats_in[slot, 3 * w + 1 : 3 * w + 2, :] for slot in range(2)
        ]
        totals = [own_sum[w]] + [stats_in[slot, 3 * w + 2 : 3 * w + 3, :] for slot in range(2)]
        best = jnp.maximum(jnp.maximum(tops[0], tops[1]), tops[2])
        factors = [jnp.exp2(top - best) for top in tops]
        mass = sum(f * m for f, m in zip(factors, masses))
        log_mass_ref[w : w + 1, :] = best * LN2 + jnp.log(mass)
        size = own_bounds[w][1].astype(jnp.float32)
        mean_ref[w : w + 1, :] = (totals[0] + totals[1] + totals[2]) * LN2 / size
        shares = [f / mass for f in factors]
        for slot in range(2):
            p_copies[slot, w].wait_recv()
        pooled = acc_own[:, half] * shares[0]
        for slot in range(2):
            pooled += parts_in[slot, w].astype(jnp.float32) * shares[1 + slot]
        pooled_ref[:, pl.ds(w * dim, dim)] = pooled.astype(jnp.bfloat16).T

    for copy in out_copies:
        copy.wait_send()


def solution(mesh):
    n_dev = mesh.shape["tm"] * mesh.shape["pb"]
    n_pb = mesh.shape["pb"]

    def local(queries, corpus, window_start, window_end):
        n_q, dim = queries.shape
        n_doc = corpus.shape[0]
        chunks = n_doc // CHUNK
        scale = SCORE_SCALE / math.sqrt(dim)
        any_spec = pl.BlockSpec(memory_space=pl.ANY)
        vmem_spec = pl.BlockSpec(memory_space=pltpu.VMEM)
        dma = pltpu.SemaphoreType.DMA
        pooled, log_mass, mean_score = pl.pallas_call(
            functools.partial(kernel, n_dev, n_pb, scale),
            out_shape=(
                jax.ShapeDtypeStruct((n_q, 2 * dim), jnp.bfloat16),
                jax.ShapeDtypeStruct((2, n_q), jnp.float32),
                jax.ShapeDtypeStruct((2, n_q), jnp.float32),
            ),
            in_specs=[any_spec] * 4,
            out_specs=(vmem_spec,) * 3,
            scratch_shapes=[
                pltpu.VMEM((n_doc, dim), jnp.bfloat16),
                pltpu.VMEM((dim, n_doc), jnp.bfloat16),
                pltpu.VMEM((2, n_doc, 2 * n_q), jnp.float32),
                pltpu.VMEM((n_q, dim), jnp.bfloat16),
                pltpu.VMEM((2, n_q, dim), jnp.bfloat16),
                pltpu.VMEM((dim, 2 * n_q), jnp.bfloat16),
                pltpu.VMEM((2, 2, n_q), jnp.int32),
                pltpu.VMEM((2, 2, 2, n_q), jnp.int32),
                pltpu.VMEM((2, 8, 2 * n_q), jnp.float32),
                pltpu.VMEM((2, 8, 2 * n_q), jnp.float32),
                pltpu.VMEM((8, 2 * n_q), jnp.float32),
                pltpu.VMEM((dim, 2 * n_q), jnp.float32),
                pltpu.VMEM((dim, 2 * n_q), jnp.float32),
                pltpu.VMEM((2, 2, dim, n_q), jnp.bfloat16),
                pltpu.VMEM((2, 2, dim, n_q), jnp.bfloat16),
                pltpu.VMEM((2, 8, n_q), jnp.float32),
                pltpu.VMEM((2, 8, n_q), jnp.float32),
                dma((chunks,)),
                dma((3,)),
                dma((2,)),
                dma((2,)),
                dma((2,)),
                dma((2,)),
                dma((2, 2)),
                dma((2, 2)),
                dma((2,)),
                dma((2,)),
            ],
            compiler_params=pltpu.CompilerParams(
                collective_id=0,
                has_side_effects=True,
                vmem_limit_bytes=60 * 1024 * 1024,
            ),
            name="window_pool",
        )(queries, corpus, window_start.T, window_end.T)
        return pooled.reshape(n_q, 2, dim), log_mass.T, mean_score.T

    rows = P(("tm", "pb"), None)
    return jax.shard_map(
        local,
        mesh=mesh,
        in_specs=(rows,) * 4,
        out_specs=(P(("tm", "pb"), None, None), rows, rows),
        check_vma=False,
    )
```

```python
import functools
import math

import jax
import jax.numpy as jnp
from jax import lax
from jax.experimental import pallas as pl
from jax.experimental.pallas import tpu as pltpu
from jax.sharding import PartitionSpec as P

NEG_FILL = -1e30
SCORE_SCALE = 3.0
LOG2E = math.log2(math.e)
MESH = pl.DeviceIdType.MESH

COPY_ROWS = 1024
OWN_ROWS = 2048
ROWS = 2048
PART_ROWS = 2048


def fold_rows(op, x):
    rows, cols = x.shape
    return op(x.reshape(rows // 8, 8, cols), axis=0)


def kernel(
    n_dev,
    n_pb,
    scale,
    q_hbm,
    c_hbm,
    start_hbm,
    stop_hbm,
    pooled_ref,
    best_ref,
    log_ref,
    total_ref,
    size_ref,
    c_v,
    c_t,
    xm,
    q_v,
    q_in,
    q_t,
    w_v,
    w_in,
    maxs,
    sums,
    tots,
    acc,
    acc_own,
    swap_out,
    swap_in,
    comb_out,
    comb_in,
    swap_stat_out,
    swap_stat_in,
    comb_stat_out,
    comb_stat_in,
    c_sem,
    local_sem,
    q_send,
    q_recv,
    w_send,
    w_recv,
    swap_send,
    swap_recv,
    comb_send,
    comb_recv,
):
    n_q, dim = q_hbm.shape
    n_doc = c_hbm.shape[0]
    me = lax.axis_index("tm") * n_pb + lax.axis_index("pb")

    def device(step):
        pos = (me + n_dev + step) % n_dev
        return (pos // n_pb, pos % n_pb)

    def send(src, dst, send_sem, recv_sem, step):
        return pltpu.make_async_remote_copy(
            src_ref=src,
            dst_ref=dst,
            send_sem=send_sem,
            recv_sem=recv_sem,
            device_id=device(step),
            device_id_type=MESH,
        )

    def c_copy(i):
        rows = pl.ds(pl.multiple_of(i * COPY_ROWS, COPY_ROWS), COPY_ROWS)
        return pltpu.make_async_copy(c_hbm.at[rows, :], c_v.at[rows, :], c_sem.at[i])

    q_copy = pltpu.make_async_copy(q_hbm, q_v, local_sem.at[0])
    start_copy = pltpu.make_async_copy(start_hbm, w_v.at[0], local_sem.at[1])
    stop_copy = pltpu.make_async_copy(stop_hbm, w_v.at[1], local_sem.at[2])
    q_copy.start()
    start_copy.start()
    stop_copy.start()
    lax.fori_loop(0, n_doc // COPY_ROWS, lambda i, _: (c_copy(i).start(), 0)[1], 0)

    barrier = pltpu.get_barrier_semaphore()
    for step in (-2, -1, 1, 2):
        pl.semaphore_signal(barrier, inc=1, device_id=device(step), device_id_type=MESH)
    pl.semaphore_wait(barrier, 4)
    q_copy.wait()
    start_copy.wait()
    stop_copy.wait()

    q_copies = []
    for slot, step in ((1, -1), (0, 1)):
        q_copies.append(send(w_v, w_in.at[slot], w_send.at[slot], w_recv.at[slot], step))
        q_copies.append(send(q_v, q_in.at[slot], q_send.at[slot], q_recv.at[slot], step))
    for copy in q_copies:
        copy.start()

    start_doc = me * n_doc

    def scores_pass(rhs, bounds, targets, cols, step_rows, first):
        width = rhs.shape[1]
        for w in range(2):
            maxs[w, :, :width] = jnp.full((8, width), NEG_FILL, jnp.float32)

        def body(i, carry):
            rows = pl.ds(pl.multiple_of(i * step_rows, step_rows), step_rows)
            if first:
                for part in range(step_rows // COPY_ROWS):
                    c_copy(i * (step_rows // COPY_ROWS) + part).wait()
            block = c_v[rows, :]
            x = jnp.dot(block, rhs[...], preferred_element_type=jnp.float32)
            if first:
                c_t[:, rows] = block.T
            doc = lax.broadcasted_iota(jnp.int32, (step_rows, width), 0)
            for w in range(2):
                low, size = bounds[w]
                offset = i * step_rows - low
                inside = (doc + offset).astype(jnp.uint32) < size.astype(jnp.uint32)
                kept = jnp.where(inside, x, NEG_FILL)
                xm[targets[w], rows, cols[w]] = kept
                maxs[w, :, :width] = jnp.maximum(maxs[w, :, :width], fold_rows(jnp.max, kept))
            return carry

        lax.fori_loop(0, n_doc // step_rows, body, 0)
        return [jnp.max(maxs[w, :, :width], axis=0, keepdims=True) for w in range(2)]

    def parts_pass(source, top, out, part, of):
        chunks = n_doc // PART_ROWS
        if part == 0:
            out[...] = jnp.zeros_like(out)
            tots[...] = jnp.zeros_like(tots)
            sums[...] = jnp.zeros_like(sums)

        def body(i, carry):
            rows = pl.ds(pl.multiple_of(i * PART_ROWS, PART_ROWS), PART_ROWS)
            kept = xm[source, rows, :]
            weights = jnp.exp2((kept - top) * (scale * LOG2E))
            tots[...] += fold_rows(jnp.sum, weights)
            sums[...] += fold_rows(jnp.sum, jnp.where(kept > 0.5 * NEG_FILL, kept, 0.0))
            low = weights.astype(jnp.bfloat16)
            for half in range(2):
                span = pl.ds(half * (dim // 2), dim // 2)
                out[span, :] += jnp.dot(c_t[span, rows], low, preferred_element_type=jnp.float32)
            return carry

        lax.fori_loop(part * chunks // of, (part + 1) * chunks // of, body, 0)
        return (
            jnp.sum(tots[...], axis=0, keepdims=True),
            jnp.sum(sums[...], axis=0, keepdims=True),
        )

    def halves(x):
        return x[:, :n_q], x[:, n_q:]

    q_t[:, pl.ds(0, n_q)] = q_v[...].T
    own_bounds = []
    for w in range(2):
        low = w_v[0, w : w + 1, :]
        own_bounds.append((low - start_doc, w_v[1, w : w + 1, :] - low))
    own_top = scores_pass(
        q_t.at[:, pl.ds(0, n_q)],
        own_bounds,
        (0, 0),
        (pl.ds(0, n_q), pl.ds(n_q, n_q)),
        OWN_ROWS,
        True,
    )
    own_tot, own_sum = map(
        halves, parts_pass(0, jnp.concatenate(own_top, axis=1), acc_own, 0, 1)
    )

    for copy in q_copies:
        copy.wait_recv()
    for slot in range(2):
        q_t[:, pl.ds(slot * n_q, n_q)] = q_in[slot].T
    bounds = []
    for w in range(2):
        low = jnp.concatenate([w_in[slot, 0, w : w + 1, :] for slot in range(2)], axis=1)
        stop = jnp.concatenate([w_in[slot, 1, w : w + 1, :] for slot in range(2)], axis=1)
        bounds.append((low - start_doc, stop - low))
    tops = scores_pass(q_t, bounds, (0, 1), (pl.ds(0, 2 * n_q),) * 2, ROWS, False)

    swaps, combs = [], []
    for w in range(2):
        swap_step, comb_step = ((-2, 1), (2, -1))[w]
        sem = (swap_send, swap_recv)
        swaps.append(
            [
                send(swap_out.at[w], swap_in.at[w], sem[0].at[w, 0], sem[1].at[w, 0], swap_step),
                send(
                    swap_stat_out.at[w],
                    swap_stat_in.at[w],
                    sem[0].at[w, 1],
                    sem[1].at[w, 1],
                    swap_step,
                ),
            ]
        )
        sem = (comb_send, comb_recv)
        combs.append(
            [
                send(comb_out.at[w], comb_in.at[w], sem[0].at[w, 0], sem[1].at[w, 0], comb_step),
                send(
                    comb_stat_out.at[w],
                    comb_stat_in.at[w],
                    sem[0].at[w, 1],
                    sem[1].at[w, 1],
                    comb_step,
                ),
            ]
        )

    def swap(w, tot, total):
        state = [halves(x) for x in (tops[w], tot, total)]
        for row, pair in enumerate(state):
            swap_stat_out[w, row : row + 1, :] = pair[w]
            comb_stat_out[w, row : row + 1, :] = pair[1 - w]
        swap_out[w] = acc[w, :, pl.ds(w * n_q, n_q)].astype(jnp.bfloat16)
        for copy in swaps[w]:
            copy.start()

    def add_up(w):
        mine = [comb_stat_out[w, row : row + 1, :] for row in range(3)]
        theirs = [swap_stat_in[w, row : row + 1, :] for row in range(3)]
        best = jnp.maximum(mine[0], theirs[0])
        factors = [jnp.exp2((x[0] - best) * (scale * LOG2E)) for x in (mine, theirs)]
        comb_out[w] = (
            acc[w, :, pl.ds((1 - w) * n_q, n_q)] * factors[0]
            + swap_in[w].astype(jnp.float32) * factors[1]
        ).astype(jnp.bfloat16)
        comb_stat_out[w, 0:1, :] = best
        comb_stat_out[w, 1:2, :] = mine[1] * factors[0] + theirs[1] * factors[1]
        comb_stat_out[w, 2:3, :] = mine[2] + theirs[2]
        for copy in combs[w]:
            copy.start()

    swap(0, *parts_pass(0, tops[0], acc.at[0], 0, 1))
    parts_pass(1, tops[1], acc.at[1], 0, 2)
    early = lax.rem(me, 4) < 2

    @pl.when(early)
    def _():
        for copy in swaps[0]:
            copy.wait_recv()
        add_up(0)

    swap(1, *parts_pass(1, tops[1], acc.at[1], 1, 2))

    @pl.when(jnp.logical_not(early))
    def _():
        for copy in swaps[0]:
            copy.wait_recv()
        add_up(0)

    for copy in swaps[1]:
        copy.wait_recv()
    add_up(1)

    for w in range(2):
        for copy in combs[w]:
            copy.wait_recv()
        far = [comb_stat_in[w, row : row + 1, :] for row in range(3)]
        best = jnp.maximum(own_top[w], far[0])
        factors = [jnp.exp2((x - best) * (scale * LOG2E)) for x in (own_top[w], far[0])]
        mass = factors[0] * own_tot[w] + factors[1] * far[1]
        best_ref[w : w + 1, :] = best * scale
        log_ref[w : w + 1, :] = jnp.log(mass)
        total_ref[w : w + 1, :] = (own_sum[w] + far[2]) * scale
        size_ref[w : w + 1, :] = own_bounds[w][1].astype(jnp.float32)
        pooled = acc_own[:, w * n_q : (w + 1) * n_q] * (factors[0] / mass)
        pooled += comb_in[w].astype(jnp.float32) * (factors[1] / mass)
        pooled_ref[:, pl.ds(w * dim, dim)] = pooled.astype(jnp.bfloat16).T

    for copy in q_copies + swaps[0] + swaps[1] + combs[0] + combs[1]:
        copy.wait_send()


def solution(mesh):
    n_dev = mesh.shape["tm"] * mesh.shape["pb"]
    n_pb = mesh.shape["pb"]

    def local(queries, corpus, window_start, window_end):
        n_q, dim = queries.shape
        n_doc = corpus.shape[0]
        scale = SCORE_SCALE / math.sqrt(dim)
        any_spec = pl.BlockSpec(memory_space=pltpu.HBM)
        vmem_spec = pl.BlockSpec(memory_space=pltpu.VMEM)
        dma = pltpu.SemaphoreType.DMA
        row = jax.ShapeDtypeStruct((2, n_q), jnp.float32)
        pooled, best, log, total, size = pl.pallas_call(
            functools.partial(kernel, n_dev, n_pb, scale),
            out_shape=(jax.ShapeDtypeStruct((n_q, 2 * dim), jnp.bfloat16),) + (row,) * 4,
            in_specs=[any_spec] * 4,
            out_specs=(vmem_spec,) * 5,
            scratch_shapes=[
                pltpu.VMEM((n_doc, dim), jnp.bfloat16),
                pltpu.VMEM((dim, n_doc), jnp.bfloat16),
                pltpu.VMEM((2, n_doc, 2 * n_q), jnp.float32),
                pltpu.VMEM((n_q, dim), jnp.bfloat16),
                pltpu.VMEM((2, n_q, dim), jnp.bfloat16),
                pltpu.VMEM((dim, 2 * n_q), jnp.bfloat16),
                pltpu.VMEM((2, 2, n_q), jnp.int32),
                pltpu.VMEM((2, 2, 2, n_q), jnp.int32),
                pltpu.VMEM((2, 8, 2 * n_q), jnp.float32),
                pltpu.VMEM((8, 2 * n_q), jnp.float32),
                pltpu.VMEM((8, 2 * n_q), jnp.float32),
                pltpu.VMEM((2, dim, 2 * n_q), jnp.float32),
                pltpu.VMEM((dim, 2 * n_q), jnp.float32),
                pltpu.VMEM((2, dim, n_q), jnp.bfloat16),
                pltpu.VMEM((2, dim, n_q), jnp.bfloat16),
                pltpu.VMEM((2, dim, n_q), jnp.bfloat16),
                pltpu.VMEM((2, dim, n_q), jnp.bfloat16),
                pltpu.VMEM((2, 8, n_q), jnp.float32),
                pltpu.VMEM((2, 8, n_q), jnp.float32),
                pltpu.VMEM((2, 8, n_q), jnp.float32),
                pltpu.VMEM((2, 8, n_q), jnp.float32),
                dma((n_doc // COPY_ROWS,)),
                dma((3,)),
                dma((2,)),
                dma((2,)),
                dma((2,)),
                dma((2,)),
                dma((2, 2)),
                dma((2, 2)),
                dma((2, 2)),
                dma((2, 2)),
            ],
            compiler_params=pltpu.CompilerParams(
                collective_id=0,
                has_side_effects=True,
                vmem_limit_bytes=62 * 1024 * 1024,
            ),
            name="window_pool",
        )(queries, corpus, window_start.T, window_end.T)
        return pooled.reshape(n_q, 2, dim), (best + log).T, (total / size).T

    rows = P(("tm", "pb"), None)
    return jax.shard_map(
        local,
        mesh=mesh,
        in_specs=(rows,) * 4,
        out_specs=(P(("tm", "pb"), None, None), rows, rows),
        check_vma=False,
    )
```

```python
import functools
import math

import jax
import jax.numpy as jnp
from jax import lax
from jax.experimental import pallas as pl
from jax.experimental.pallas import tpu as pltpu
from jax.sharding import PartitionSpec as P

NEG_FILL = -1e30
SCORE_SCALE = 3.0
LOG2E = math.log2(math.e)
MESH = pl.DeviceIdType.MESH

LINE = 32
COPY_ROWS = 1024
OWN_ROWS = 2048
ROWS = 2048
PART_ROWS = 2048


def fold_rows(op, x):
    rows, cols = x.shape
    return op(x.reshape(rows // 8, 8, cols), axis=0)


def kernel(
    n_dev,
    n_pb,
    line,
    scale,
    q_hbm,
    c_hbm,
    start_hbm,
    stop_hbm,
    pooled_ref,
    best_ref,
    log_ref,
    total_ref,
    size_ref,
    c_v,
    c_t,
    xm,
    q_v,
    q_in,
    q_t,
    w_v,
    w_in,
    maxs,
    sums,
    tots,
    acc,
    acc_own,
    swap_out,
    swap_in,
    comb_out,
    comb_in,
    swap_stat_out,
    swap_stat_in,
    comb_stat_out,
    comb_stat_in,
    far_in,
    far_stat_in,
    far_sum,
    c_sem,
    local_sem,
    q_send,
    q_recv,
    w_send,
    w_recv,
    swap_send,
    swap_recv,
    comb_send,
    comb_recv,
    far_recv,
):
    n_q, dim = q_hbm.shape
    n_doc = c_hbm.shape[0]
    me = lax.axis_index("tm") * n_pb + lax.axis_index("pb")

    def device(step):
        pos = (me + n_dev + step) % n_dev
        return (pos // n_pb, pos % n_pb)

    def send(src, dst, send_sem, recv_sem, step):
        return pltpu.make_async_remote_copy(
            src_ref=src,
            dst_ref=dst,
            send_sem=send_sem,
            recv_sem=recv_sem,
            device_id=device(step),
            device_id_type=MESH,
        )

    def c_copy(i):
        rows = pl.ds(pl.multiple_of(i * COPY_ROWS, COPY_ROWS), COPY_ROWS)
        return pltpu.make_async_copy(c_hbm.at[rows, :], c_v.at[rows, :], c_sem.at[i])

    q_copy = pltpu.make_async_copy(q_hbm, q_v, local_sem.at[0])
    start_copy = pltpu.make_async_copy(start_hbm, w_v.at[0], local_sem.at[1])
    stop_copy = pltpu.make_async_copy(stop_hbm, w_v.at[1], local_sem.at[2])
    q_copy.start()
    start_copy.start()
    stop_copy.start()
    lax.fori_loop(0, n_doc // COPY_ROWS, lambda i, _: (c_copy(i).start(), 0)[1], 0)

    def in_array(step):
        return jnp.logical_and(me + step >= 0, me + step < n_dev)

    def same_line(step):
        return jnp.logical_and(in_array(step), (me + n_dev) // line == (me + n_dev + step) // line)

    peers = {-2: same_line(-2), -1: in_array(-1), 1: in_array(1), 2: same_line(2)}
    barrier = pltpu.get_barrier_semaphore()
    for step, there in peers.items():

        @pl.when(there)
        def _(step=step):
            pl.semaphore_signal(barrier, inc=1, device_id=device(step), device_id_type=MESH)

    pl.semaphore_wait(barrier, sum(there.astype(jnp.int32) for there in peers.values()))
    q_copy.wait()
    start_copy.wait()
    stop_copy.wait()

    q_copies = [[], []]
    for slot, step in ((1, -1), (0, 1)):
        q_copies[slot] = [
            send(w_v, w_in.at[slot], w_send.at[slot], w_recv.at[slot], step),
            send(q_v, q_in.at[slot], q_send.at[slot], q_recv.at[slot], step),
        ]

        @pl.when(peers[step])
        def _(slot=slot):
            for copy in q_copies[slot]:
                copy.start()

        @pl.when(jnp.logical_not(peers[step]))
        def _(slot=slot):
            q_in[1 - slot] = q_v[...]
            w_in[1 - slot] = w_v[...]

    start_doc = me * n_doc

    def scores_pass(rhs, bounds, targets, cols, step_rows, first):
        width = rhs.shape[1]
        for w in range(2):
            maxs[w, :, :width] = jnp.full((8, width), NEG_FILL, jnp.float32)

        def body(i, carry):
            rows = pl.ds(pl.multiple_of(i * step_rows, step_rows), step_rows)
            if first:
                for part in range(step_rows // COPY_ROWS):
                    c_copy(i * (step_rows // COPY_ROWS) + part).wait()
            block = c_v[rows, :]
            x = jnp.dot(block, rhs[...], preferred_element_type=jnp.float32)
            if first:
                c_t[:, rows] = block.T
            doc = lax.broadcasted_iota(jnp.int32, (step_rows, width), 0)
            for w in range(2):
                low, size = bounds[w]
                offset = i * step_rows - low
                inside = (doc + offset).astype(jnp.uint32) < size.astype(jnp.uint32)
                kept = jnp.where(inside, x, NEG_FILL)
                xm[targets[w], rows, cols[w]] = kept
                maxs[w, :, :width] = jnp.maximum(maxs[w, :, :width], fold_rows(jnp.max, kept))
            return carry

        lax.fori_loop(0, n_doc // step_rows, body, 0)
        return [jnp.max(maxs[w, :, :width], axis=0, keepdims=True) for w in range(2)]

    def parts_pass(source, top, out, part, of):
        chunks = n_doc // PART_ROWS
        if part == 0:
            out[...] = jnp.zeros_like(out)
            tots[...] = jnp.zeros_like(tots)
            sums[...] = jnp.zeros_like(sums)

        def body(i, carry):
            rows = pl.ds(pl.multiple_of(i * PART_ROWS, PART_ROWS), PART_ROWS)
            kept = xm[source, rows, :]
            weights = jnp.exp2((kept - top) * (scale * LOG2E))
            tots[...] += fold_rows(jnp.sum, weights)
            sums[...] += fold_rows(jnp.sum, jnp.where(kept > 0.5 * NEG_FILL, kept, 0.0))
            low = weights.astype(jnp.bfloat16)
            for half in range(2):
                span = pl.ds(half * (dim // 2), dim // 2)
                out[span, :] += jnp.dot(c_t[span, rows], low, preferred_element_type=jnp.float32)
            return carry

        lax.fori_loop(part * chunks // of, (part + 1) * chunks // of, body, 0)
        return (
            jnp.sum(tots[...], axis=0, keepdims=True),
            jnp.sum(sums[...], axis=0, keepdims=True),
        )

    def halves(x):
        return x[:, :n_q], x[:, n_q:]

    q_t[:, pl.ds(0, n_q)] = q_v[...].T
    own_bounds = []
    for w in range(2):
        low = w_v[0, w : w + 1, :]
        own_bounds.append((low - start_doc, w_v[1, w : w + 1, :] - low))
    own_top = scores_pass(
        q_t.at[:, pl.ds(0, n_q)],
        own_bounds,
        (0, 0),
        (pl.ds(0, n_q), pl.ds(n_q, n_q)),
        OWN_ROWS,
        True,
    )
    own_tot, own_sum = map(
        halves, parts_pass(0, jnp.concatenate(own_top, axis=1), acc_own, 0, 1)
    )

    for slot, step in ((0, -1), (1, 1)):

        @pl.when(peers[step])
        def _(slot=slot):
            for copy in q_copies[slot]:
                copy.wait_recv()

    for slot in range(2):
        q_t[:, pl.ds(slot * n_q, n_q)] = q_in[slot].T
    bounds = []
    for w in range(2):
        low = jnp.concatenate([w_in[slot, 0, w : w + 1, :] for slot in range(2)], axis=1)
        stop = jnp.concatenate([w_in[slot, 1, w : w + 1, :] for slot in range(2)], axis=1)
        bounds.append((low - start_doc, stop - low))
    tops = scores_pass(q_t, bounds, (0, 1), (pl.ds(0, 2 * n_q),) * 2, ROWS, False)

    swaps, combs, straights, fars = [], [], [], []

    def state_copies(out, stat_out, into, stat_into, sems, w, step):
        return [
            send(out.at[w], into.at[w], sems[0].at[w, 0], sems[1].at[w, 0], step),
            send(stat_out.at[w], stat_into.at[w], sems[0].at[w, 1], sems[1].at[w, 1], step),
        ]

    into_comb = (comb_in, comb_stat_in)
    into_far = (far_in, far_stat_in)
    for w in range(2):
        swap_step, comb_step = ((-2, 1), (2, -1))[w]
        from_swap = (swap_out, swap_stat_out)
        from_comb = (comb_out, comb_stat_out)
        swap_sems, comb_sems = (swap_send, swap_recv), (comb_send, comb_recv)
        owner_sems, far_sems = (swap_send, comb_recv), (swap_send, far_recv)
        swaps.append(
            state_copies(*from_swap, swap_in, swap_stat_in, swap_sems, w, swap_step)
        )
        combs.append(state_copies(*from_comb, *into_comb, comb_sems, w, comb_step))
        straights.append(state_copies(*from_swap, *into_comb, owner_sems, w, swap_step // 2))
        fars.append(
            (
                state_copies(*from_swap, *into_far, far_sems, w, swap_step // 2),
                state_copies(*from_comb, *into_far, (comb_send, far_recv), w, comb_step),
            )
        )

    def start(copies, when):
        @pl.when(when)
        def _():
            for copy in copies:
                copy.start()

    def wait_recv(copies, when):
        @pl.when(when)
        def _():
            for copy in copies:
                copy.wait_recv()

    def swap(w, tot, total):
        state = [halves(x) for x in (tops[w], tot, total)]
        for row, pair in enumerate(state):
            swap_stat_out[w, row : row + 1, :] = pair[w]
            comb_stat_out[w, row : row + 1, :] = pair[1 - w]
        swap_out[w] = acc[w, :, pl.ds(w * n_q, n_q)].astype(jnp.bfloat16)
        far_step = (-2, 2)[w]
        owner_step = far_step // 2
        start(swaps[w], peers[far_step])
        near = jnp.logical_and(same_line(owner_step), jnp.logical_not(peers[far_step]))
        start(straights[w], near)
        start(fars[w][0], jnp.logical_and(peers[owner_step], jnp.logical_not(same_line(owner_step))))

    def add_up(w):
        paired = peers[(2, -2)[w]]
        owner_step = (1, -1)[w]
        mine = [comb_stat_out[w, row : row + 1, :] for row in range(3)]
        mine_part = pl.ds((1 - w) * n_q, n_q)

        @pl.when(paired)
        def _():
            for copy in swaps[w]:
                copy.wait_recv()
            theirs = [swap_stat_in[w, row : row + 1, :] for row in range(3)]
            best = jnp.maximum(mine[0], theirs[0])
            factors = [jnp.exp2((x[0] - best) * (scale * LOG2E)) for x in (mine, theirs)]
            comb_out[w] = (
                acc[w, :, mine_part] * factors[0] + swap_in[w].astype(jnp.float32) * factors[1]
            ).astype(jnp.bfloat16)
            comb_stat_out[w, 0:1, :] = best
            comb_stat_out[w, 1:2, :] = mine[1] * factors[0] + theirs[1] * factors[1]
            comb_stat_out[w, 2:3, :] = mine[2] + theirs[2]

        @pl.when(jnp.logical_not(paired))
        def _():
            comb_out[w] = acc[w, :, mine_part].astype(jnp.bfloat16)

        start(combs[w], same_line(owner_step))
        start(
            fars[w][1], jnp.logical_and(peers[owner_step], jnp.logical_not(same_line(owner_step)))
        )

    swap(0, *parts_pass(0, tops[0], acc.at[0], 0, 1))
    early = jnp.logical_or(lax.rem(me, 4) < 2, jnp.logical_not(peers[2]))
    parts_pass(1, tops[1], acc.at[1], 0, 2)

    @pl.when(early)
    def _():
        add_up(0)

    swap(1, *parts_pass(1, tops[1], acc.at[1], 1, 2))

    @pl.when(jnp.logical_not(early))
    def _():
        add_up(0)

    add_up(1)

    edge = jnp.logical_or(
        jnp.logical_and(peers[-1], jnp.logical_not(same_line(-1))),
        jnp.logical_and(peers[1], jnp.logical_not(same_line(1))),
    )
    for w in range(2):
        wait_recv(combs[w], me >= 0)
        wait_recv(fars[w][1], edge)

        @pl.when(edge)
        def _(w=w):
            mine = [comb_stat_in[w, row : row + 1, :] for row in range(3)]
            theirs = [far_stat_in[w, row : row + 1, :] for row in range(3)]
            best = jnp.maximum(mine[0], theirs[0])
            factors = [jnp.exp2((x[0] - best) * (scale * LOG2E)) for x in (mine, theirs)]
            acc[w, :, pl.ds(0, n_q)] = (
                comb_in[w].astype(jnp.float32) * factors[0]
                + far_in[w].astype(jnp.float32) * factors[1]
            )
            far_sum[w, 0:1, :] = best
            far_sum[w, 1:2, :] = mine[1] * factors[0] + theirs[1] * factors[1]
            far_sum[w, 2:3, :] = mine[2] + theirs[2]

        @pl.when(jnp.logical_not(edge))
        def _(w=w):
            acc[w, :, pl.ds(0, n_q)] = comb_in[w].astype(jnp.float32)
            far_sum[w] = comb_stat_in[w]

        far = [far_sum[w, row : row + 1, :] for row in range(3)]
        best = jnp.maximum(own_top[w], far[0])
        factors = [jnp.exp2((x - best) * (scale * LOG2E)) for x in (own_top[w], far[0])]
        mass = factors[0] * own_tot[w] + factors[1] * far[1]
        best_ref[w : w + 1, :] = best * scale
        log_ref[w : w + 1, :] = jnp.log(mass)
        total_ref[w : w + 1, :] = (own_sum[w] + far[2]) * scale
        size_ref[w : w + 1, :] = own_bounds[w][1].astype(jnp.float32)
        pooled = acc_own[:, w * n_q : (w + 1) * n_q] * (factors[0] / mass)
        pooled += acc[w, :, pl.ds(0, n_q)] * (factors[1] / mass)
        pooled_ref[:, pl.ds(w * dim, dim)] = pooled.astype(jnp.bfloat16).T

    for slot, step in ((1, -1), (0, 1)):

        @pl.when(peers[step])
        def _(slot=slot):
            for copy in q_copies[slot]:
                copy.wait_send()

    for w in range(2):
        for copies, step in ((swaps[w], (-1, 1)[w]), (combs[w], (1, -1)[w])):

            @pl.when(peers[step])
            def _(copies=copies):
                for copy in copies:
                    copy.wait_send()


def solution(mesh):
    n_dev = mesh.shape["tm"] * mesh.shape["pb"]
    n_pb = mesh.shape["pb"]

    def local(queries, corpus, window_start, window_end):
        n_q, dim = queries.shape
        n_doc = corpus.shape[0]
        scale = SCORE_SCALE / math.sqrt(dim)
        any_spec = pl.BlockSpec(memory_space=pltpu.HBM)
        vmem_spec = pl.BlockSpec(memory_space=pltpu.VMEM)
        dma = pltpu.SemaphoreType.DMA
        row = jax.ShapeDtypeStruct((2, n_q), jnp.float32)
        pooled, best, log, total, size = pl.pallas_call(
            functools.partial(kernel, n_dev, n_pb, min(LINE, n_dev), scale),
            out_shape=(jax.ShapeDtypeStruct((n_q, 2 * dim), jnp.bfloat16),) + (row,) * 4,
            in_specs=[any_spec] * 4,
            out_specs=(vmem_spec,) * 5,
            scratch_shapes=[
                pltpu.VMEM((n_doc, dim), jnp.bfloat16),
                pltpu.VMEM((dim, n_doc), jnp.bfloat16),
                pltpu.VMEM((2, n_doc, 2 * n_q), jnp.float32),
                pltpu.VMEM((n_q, dim), jnp.bfloat16),
                pltpu.VMEM((2, n_q, dim), jnp.bfloat16),
                pltpu.VMEM((dim, 2 * n_q), jnp.bfloat16),
                pltpu.VMEM((2, 2, n_q), jnp.int32),
                pltpu.VMEM((2, 2, 2, n_q), jnp.int32),
                pltpu.VMEM((2, 8, 2 * n_q), jnp.float32),
                pltpu.VMEM((8, 2 * n_q), jnp.float32),
                pltpu.VMEM((8, 2 * n_q), jnp.float32),
                pltpu.VMEM((2, dim, 2 * n_q), jnp.float32),
                pltpu.VMEM((dim, 2 * n_q), jnp.float32),
                pltpu.VMEM((2, dim, n_q), jnp.bfloat16),
                pltpu.VMEM((2, dim, n_q), jnp.bfloat16),
                pltpu.VMEM((2, dim, n_q), jnp.bfloat16),
                pltpu.VMEM((2, dim, n_q), jnp.bfloat16),
                pltpu.VMEM((2, 8, n_q), jnp.float32),
                pltpu.VMEM((2, 8, n_q), jnp.float32),
                pltpu.VMEM((2, 8, n_q), jnp.float32),
                pltpu.VMEM((2, 8, n_q), jnp.float32),
                pltpu.VMEM((2, dim, n_q), jnp.bfloat16),
                pltpu.VMEM((2, 8, n_q), jnp.float32),
                pltpu.VMEM((2, 8, n_q), jnp.float32),
                dma((n_doc // COPY_ROWS,)),
                dma((3,)),
                dma((2,)),
                dma((2,)),
                dma((2,)),
                dma((2,)),
                dma((2, 2)),
                dma((2, 2)),
                dma((2, 2)),
                dma((2, 2)),
                dma((2, 2)),
            ],
            compiler_params=pltpu.CompilerParams(
                collective_id=0,
                has_side_effects=True,
                vmem_limit_bytes=62 * 1024 * 1024,
            ),
            name="window_pool",
        )(queries, corpus, window_start.T, window_end.T)
        return pooled.reshape(n_q, 2, dim), (best + log).T, (total / size).T

    rows = P(("tm", "pb"), None)
    return jax.shard_map(
        local,
        mesh=mesh,
        in_specs=(rows,) * 4,
        out_specs=(P(("tm", "pb"), None, None), rows, rows),
        check_vma=False,
    )
```
